32 devices in a mesh: band: 8 (over z, x), space: 4 (over y, core).
Axes of the slice: x: 2, y: 2, z: 4, core: 2. Of those that a mesh axis runs over, the one named last changes fastest.
Arguments:
- orbitals: bfloat16 [64, 64, 160, 128], P('band', None, 'space'), may hold values from -8.5 to 8.5
- occupations: float32 [64], P('band'), may hold values from 0.07 to 2.5
Outputs:
- potential: float32 [64, 160, 128], P('band', 'space')
The draws below stay inside these ranges and needn't reach their ends.
All inputs are finite; a program needn't handle non-finite values.
Results may differ from the reference program's by a relative error of at most 0.0003.
Values sent between devices are 32-bit elements; how exact they have to be, the bound alone decides.
A program may use at most 64 MiB of HBM per device.

```python
import math
import jax
import jax.numpy as jnp
from jax import lax

NY = 128
ITERS = 3
BANDS = 64
X = 64
NZ = 160


def draw_orbitals(key, part):
    first = jax.random.fold_in(jax.random.fold_in(key, 11), 0)
    shape = (BANDS, X, NZ, NY)
    position = jnp.arange(X, dtype=jnp.float32) / (X - 1)
    envelope = jnp.sqrt(0.5 + 1.5 * position)[None, :, None, None]
    base = jnp.clip(jax.random.normal(first, shape, jnp.float32), -6.0, 6.0)
    return (base * envelope).astype(jnp.bfloat16)


def draw_occupations(key, part):
    level = jnp.arange(BANDS, dtype=jnp.float32) / BANDS
    fermi = 2.0 / (1.0 + jnp.exp(4.0 * level - 1.5))
    factor = jax.random.uniform(jax.random.fold_in(key, 23), (BANDS,), jnp.float32, 0.7, 1.3)
    return (fermi * factor).astype(jnp.float32)


def setup_inputs(seed: int = 0) -> dict:
    splits = jax.random.split(jax.random.key(seed), 3)
    orbitals = draw_orbitals(jax.random.fold_in(splits[2], 71), 0)
    occupations = draw_occupations(jax.random.fold_in(splits[2], 71), 0)
    return dict(orbitals=orbitals, occupations=occupations)


four_pi = 4.0 * math.pi


def stencil(padded):
    center = padded[2:-2, 2:-2, 2:-2]
    near = padded[3:-1, 2:-2, 2:-2] + padded[1:-3, 2:-2, 2:-2]
    near = near + padded[2:-2, 3:-1, 2:-2] + padded[2:-2, 1:-3, 2:-2]
    near = near + padded[2:-2, 2:-2, 3:-1] + padded[2:-2, 2:-2, 1:-3]
    distant = padded[4:, 2:-2, 2:-2] + padded[:-4, 2:-2, 2:-2]
    distant = distant + padded[2:-2, 4:, 2:-2] + padded[2:-2, :-4, 2:-2]
    distant = distant + padded[2:-2, 2:-2, 4:] + padded[2:-2, 2:-2, :-4]
    return 7.5 * center - (4.0 / 3.0) * near + (1.0 / 12.0) * distant


def reference(orbitals, occupations):
    def accumulate(index, total):
        wave = lax.dynamic_index_in_dim(orbitals, index, 0, keepdims=False).astype(jnp.float32)
        return total + occupations[index] * wave * wave

    start = jnp.zeros(orbitals.shape[1:], jnp.float32)
    density = lax.fori_loop(0, orbitals.shape[0], accumulate, start) / BANDS
    source = four_pi * density
    potential = jnp.zeros_like(source)
    residual, direction = source, source
    norm_now = jnp.sum(residual * residual)
    for step in range(ITERS):
        image = stencil(jnp.pad(direction, 2))
        alpha = norm_now / jnp.sum(direction * image)
        potential = potential + alpha * direction
        residual = residual - alpha * image
        norm_next = jnp.sum(residual * residual)
        direction = residual + (norm_next / norm_now) * direction
        norm_now = norm_next
    return potential
```

```python
import functools
import math

import jax
import jax.numpy as jnp
from jax import lax
from jax.experimental import pallas as pl
from jax.experimental.pallas import tpu as pltpu
from jax.sharding import PartitionSpec as P

MESH = pl.DeviceIdType.MESH
REACH = 2
DEEP = 3 * REACH
EDGE = 8
CORNER = 2 * REACH
DIRECTIONS = ((1, 0), (-1, 0), (0, 1), (0, -1), (1, 1), (1, -1), (-1, 1), (-1, -1))


def permuted(position, order, stages):
    offset = 0
    for s, bit in enumerate(order):
        digit = (position // (1 << (stages - 1 - s))) % 2
        offset = offset + digit * (1 << bit)
    return offset


def flipped(index, offset, stages):
    total = 0
    for k in range(stages):
        a, b = (index // (1 << k)) % 2, (offset // (1 << k)) % 2
        total = total + ((a + b) % 2) * (1 << k)
    return total


def kernel(bands, spaces, groups, bands_total, chunks, orders, occ_ref, orb_ref, out_ref,
           held, acc, got, field, first, second, mine, theirs, band_sum, space_sums,
           load_sem, rs_send, rs_recv, halo_send, halo_recv, mb_send, mb_recv, ms_send, ms_recv):
    b, s = lax.axis_index("band"), lax.axis_index("space")
    stages = len(orders[0])
    planes, rows, lanes = out_ref.shape
    part = planes // chunks
    tall = rows + 2 * EDGE

    loads = {}
    for q in range(bands - 1, -1, -1):
        share = flipped(b, q, stages)
        loads[q] = pltpu.make_async_copy(
            orb_ref.at[:, pl.ds(share * planes, planes)], held.at[q], load_sem.at[q])
        loads[q].start()

    field[...] = jnp.zeros_like(field)

    barrier = pltpu.get_barrier_semaphore()
    greet = [((b + k) % bands, s) for k in range(1, bands)]
    greet += [(b, (s + k) % spaces) for k in range(1, spaces)]
    greet += [((b + db + bands) % bands, (s + ds + spaces) % spaces)
              for db, ds in DIRECTIONS if db and ds]
    for peer in greet:
        pl.semaphore_signal(barrier, inc=1, device_id=peer, device_id_type=MESH)

    for q in range(bands):
        loads[q].wait()

    weights = [occ_ref[k] for k in range(groups)]

    def density(c, low, high):
        def body(i, _):
            position = low + i // part
            plane = i % part
            offset = permuted(position, orders[c], stages)
            total = jnp.zeros((rows, lanes), jnp.float32)
            for k in range(groups):
                wave = held[offset, k, c * part + plane].astype(jnp.float32)
                total = total + (weights[k] * wave) * wave
            acc[c, position, plane] = total
            return 0
        lax.fori_loop(0, (high - low) * part, body, 0)

    def hop(c, stage):
        half = bands >> (stage + 1)
        bit = 1 << orders[c][stage]
        peer = b + bit * (1 - 2 * ((b // bit) % 2))
        return pltpu.make_async_remote_copy(
            src_ref=acc.at[c, pl.ds(half, half)], dst_ref=got.at[c, pl.ds(half, half)],
            send_sem=rs_send.at[c, stage], recv_sem=rs_recv.at[c, stage],
            device_id=(peer, s), device_id_type=MESH)

    hops = {(c, t): hop(c, t) for c in range(chunks) for t in range(stages)}
    for c in range(chunks):
        density(c, bands // 2, bands)
        if c == 0:
            pl.semaphore_wait(barrier, len(greet))
        hops[c, 0].start()
    for c in range(chunks):
        density(c, 0, bands // 2)

    scale = 4.0 * math.pi / bands_total
    order = sorted(hops, key=lambda ct: (ct[0] // 2 + ct[1], -ct[1], ct[0]))
    for c, t in order:
        half = bands >> (t + 1)
        hops[c, t].wait_recv()

        if t + 1 < stages:
            quarter = half // 2

            def add(i, _):
                position, plane = i // part, i % part
                acc[c, position, plane] = acc[c, position, plane] + got[c, half + position, plane]
                return 0
            lax.fori_loop(quarter * part, half * part, add, 0)
            hops[c, t + 1].start()
            lax.fori_loop(0, quarter * part, add, 0)
        else:
            for plane in range(part):
                field[DEEP + c * part + plane, EDGE:EDGE + rows] = scale * (
                    acc[c, 0, plane] + got[c, 1, plane])

    def span(d, size, width, halo):
        if d > 0:
            return size + halo - width, halo - width
        return halo, size + halo

    halos = []
    for i, (db, ds) in enumerate(DIRECTIONS):
        deep = DEEP if not ds else (CORNER if db else planes)
        wide = EDGE if ds else rows
        src_p, dst_p = span(db, planes, deep, DEEP) if db else (DEEP, DEEP)
        src_r, dst_r = span(ds, rows, wide, EDGE) if ds else (EDGE, EDGE)
        to = ((b + db + bands) % bands, (s + ds + spaces) % spaces)
        copy = pltpu.make_async_remote_copy(
            src_ref=field.at[pl.ds(src_p, deep), pl.ds(src_r, wide)],
            dst_ref=field.at[pl.ds(dst_p, deep), pl.ds(dst_r, wide)],
            send_sem=halo_send.at[i], recv_sem=halo_recv.at[i],
            device_id=to, device_id_type=MESH)

        def inside(x, y, db=db, ds=ds):
            ok = None
            for d, v, n in ((db, x, bands), (ds, y, spaces)):
                if d:
                    here = (v + d >= 0) & (v + d < n)
                    ok = here if ok is None else ok & here
            return ok
        sends = inside(b, s)
        takes = None
        for d, v, n in ((db, b, bands), (ds, s, spaces)):
            if d:
                here = (v - d >= 0) & (v - d < n)
                takes = here if takes is None else takes & here
        pl.when(sends)(copy.start)
        halos.append((copy, sends, takes))
    for copy, sends, takes in halos:
        pl.when(takes)(copy.wait_recv)
    for copy, sends, takes in halos:
        pl.when(sends)(copy.wait_send)

    row = lax.broadcasted_iota(jnp.int32, (tall, lanes), 0)
    lane = lax.broadcasted_iota(jnp.int32, (tall, lanes), 1)
    low_row = jnp.where(s == 0, EDGE, 0)
    high_row = jnp.where(s == spaces - 1, EDGE + rows, tall)
    rows_in = ((row >= low_row) & (row < high_row)).astype(jnp.float32)
    near, far = -4.0 / 3.0, 1.0 / 12.0
    lane_terms = [(shift % lanes, jnp.where((lane - shift >= 0) & (lane - shift < lanes), w, 0.0))
                  for shift, w in ((1, near), (-1, near), (2, far), (-2, far))]
    low_plane = jnp.where(b == 0, DEEP, 0)
    high_plane = jnp.where(b == bands - 1, DEEP + planes, planes + 2 * DEEP)

    def apply(ref, p):
        v = ref[p]
        ones = ref[p - 1] + ref[p + 1] + pltpu.roll(v, 1, 0) + pltpu.roll(v, tall - 1, 0)
        twos = ref[p - 2] + ref[p + 2] + pltpu.roll(v, 2, 0) + pltpu.roll(v, tall - 2, 0)
        total = 7.5 * v + near * ones + far * twos
        for shift, coefficient in lane_terms:
            total = total + coefficient * pltpu.roll(v, shift, 1)
        return total

    def step(src, dst):
        def body(p, _):
            here = jnp.where((p >= low_plane) & (p < high_plane), 1.0, 0.0)
            dst[p] = apply(src, p) * (rows_in * here)
            return 0
        return body

    lax.fori_loop(REACH, planes + 2 * DEEP - REACH, step(field, first), 0)
    lax.fori_loop(2 * REACH, planes + 2 * DEEP - 2 * REACH, step(first, second), 0)

    def fold(x):
        x = x[EDGE:EDGE + rows]
        total = x[0:8]
        for k in range(8, rows, 8):
            total = total + x[k:k + 8]
        return total

    def moments(p, sums):
        w0, w1, w2 = field[p], first[p], second[p]
        w3 = apply(second, p)
        terms = (w0 * w0, w0 * w1, w1 * w1, w1 * w2, w2 * w2, w2 * w3)
        return tuple(x + fold(y) for x, y in zip(sums, terms))

    sums = lax.fori_loop(DEEP, DEEP + planes, moments,
                         tuple(jnp.zeros((8, lanes), jnp.float32) for _ in range(6)))
    packed = [jnp.sum(x, axis=0, keepdims=True) for x in sums]
    packed = jnp.concatenate(packed + [jnp.zeros((2, lanes), jnp.float32)], axis=0)
    mine[...] = packed
    copies = []
    for k in range(1, bands):
        copies.append(pltpu.make_async_remote_copy(
            src_ref=mine, dst_ref=theirs.at[b], send_sem=mb_send.at[k], recv_sem=mb_recv.at[k],
            device_id=((b + k) % bands, s), device_id_type=MESH))
        copies[-1].start()
    theirs[b] = packed
    for copy in copies:
        copy.wait_recv()
    total = theirs[0]
    for k in range(1, bands):
        total = total + theirs[k]
    band_sum[...] = total
    across = []
    for k in range(1, spaces):
        across.append(pltpu.make_async_remote_copy(
            src_ref=band_sum, dst_ref=space_sums.at[s], send_sem=ms_send.at[k],
            recv_sem=ms_recv.at[k], device_id=(b, (s + k) % spaces), device_id_type=MESH))
        across[-1].start()
    space_sums[s] = total
    for copy in across:
        copy.wait_recv()
    total = space_sums[0]
    for k in range(1, spaces):
        total = total + space_sums[k]
    total = jnp.sum(total, axis=1, keepdims=True)
    mu = [total[k:k + 1] for k in range(6)]

    def form(c, shift):
        value = None
        for i in range(len(c)):
            for j in range(i, len(c)):
                term = c[i] * c[j] * mu[i + j + shift]
                term = term if i == j else 2.0 * term
                value = term if value is None else value + term
        return value

    alpha0 = mu[0] / mu[1]
    r1 = [jnp.ones_like(alpha0), -alpha0]
    rr1 = form(r1, 0)
    beta0 = rr1 / mu[0]
    d1 = [1.0 + beta0, -alpha0]
    alpha1 = rr1 / form(d1, 1)
    r2 = [r1[0], r1[1] - alpha1 * d1[0], -alpha1 * d1[1]]
    rr2 = form(r2, 0)
    beta1 = rr2 / rr1
    d2 = [r2[0] + beta1 * d1[0], r2[1] + beta1 * d1[1], r2[2]]
    alpha2 = rr2 / form(d2, 1)
    c0 = alpha0 + alpha1 * d1[0] + alpha2 * d2[0]
    c1 = alpha1 * d1[1] + alpha2 * d2[1]
    c2 = alpha2 * d2[2]

    for p in range(planes):
        at = (DEEP + p, slice(EDGE, EDGE + rows))
        out_ref[p] = c0 * field[at] + c1 * first[at] + c2 * second[at]

    for c, t in order:
        hops[c, t].wait_send()
    for copy in copies + across:
        copy.wait_send()


def solution(mesh):
    bands, spaces = mesh.shape["band"], mesh.shape["space"]
    stages = bands.bit_length() - 1

    def local(orbitals, occupations):
        groups, length, rows, lanes = orbitals.shape
        planes = length // bands
        chunks = 4
        part = planes // chunks
        forward = list(range(stages))
        half = stages // 2
        swapped = forward[half:half + 1] + forward[:half] + forward[half + 1:]
        orders = [forward if c % 2 == 0 else swapped for c in range(chunks)]
        body = functools.partial(kernel, bands, spaces, groups, groups * bands, chunks, orders)
        tall, deep = rows + 2 * EDGE, planes + 2 * DEEP
        f32 = jnp.float32
        return pl.pallas_call(
            body,
            out_shape=jax.ShapeDtypeStruct((planes, rows, lanes), f32),
            in_specs=[pl.BlockSpec(memory_space=pltpu.SMEM), pl.BlockSpec(memory_space=pl.ANY)],
            out_specs=pl.BlockSpec(memory_space=pltpu.VMEM),
            scratch_shapes=[
                pltpu.VMEM((bands, groups, planes, rows, lanes), orbitals.dtype),
                pltpu.VMEM((chunks, bands, part, rows, lanes), f32),
                pltpu.VMEM((chunks, bands, part, rows, lanes), f32),
                pltpu.VMEM((deep, tall, lanes), f32),
                pltpu.VMEM((deep, tall, lanes), f32),
                pltpu.VMEM((deep, tall, lanes), f32),
                pltpu.VMEM((8, lanes), f32),
                pltpu.VMEM((bands, 8, lanes), f32),
                pltpu.VMEM((8, lanes), f32),
                pltpu.VMEM((spaces, 8, lanes), f32),
                pltpu.SemaphoreType.DMA((bands,)),
                pltpu.SemaphoreType.DMA((chunks, stages)),
                pltpu.SemaphoreType.DMA((chunks, stages)),
                pltpu.SemaphoreType.DMA((len(DIRECTIONS),)),
                pltpu.SemaphoreType.DMA((len(DIRECTIONS),)),
                pltpu.SemaphoreType.DMA((bands,)),
                pltpu.SemaphoreType.DMA((bands,)),
                pltpu.SemaphoreType.DMA((spaces,)),
                pltpu.SemaphoreType.DMA((spaces,)),
            ],
            compiler_params=pltpu.CompilerParams(
                collective_id=0, has_side_effects=True, vmem_limit_bytes=48 * 1024 * 1024),
        )(occupations, orbitals)

    in_specs = (P("band", None, "space", None), P("band"))
    out_specs = P("band", "space", None)
    return jax.shard_map(local, mesh=mesh, in_specs=in_specs, out_specs=out_specs, check_vma=False)
```

```python
import functools
import math

import jax
import jax.numpy as jnp
from jax import lax
from jax.experimental import pallas as pl
from jax.experimental.pallas import tpu as pltpu
from jax.sharding import PartitionSpec as P

MESH = pl.DeviceIdType.MESH
REACH = 2
DEEP = 3 * REACH
EDGE = 8
CORNER = 2 * REACH
DIRECTIONS = ((1, 0), (-1, 0), (0, 1), (0, -1), (1, 1), (1, -1), (-1, 1), (-1, -1))


def permuted(position, order, stages):
    offset = 0
    for s, bit in enumerate(order):
        digit = (position // (1 << (stages - 1 - s))) % 2
        offset = offset + digit * (1 << bit)
    return offset


def flipped(index, offset, stages):
    total = 0
    for k in range(stages):
        a, b = (index // (1 << k)) % 2, (offset // (1 << k)) % 2
        total = total + ((a + b) % 2) * (1 << k)
    return total


def kernel(bands, spaces, groups, bands_total, chunks, orders, occ_ref, orb_ref, out_ref,
           held, acc, got, field, first, second, mine, theirs,
           load_sem, rs_send, rs_recv, halo_send, halo_recv, mb_send, mb_recv, ready):
    b, s = lax.axis_index("band"), lax.axis_index("space")
    stages = len(orders[0])
    planes, rows, lanes = out_ref.shape
    part = planes // chunks
    tall = rows + 2 * EDGE

    loads = {}
    for q in range(bands - 1, -1, -1):
        share = flipped(b, q, stages)
        loads[q] = pltpu.make_async_copy(
            orb_ref.at[:, pl.ds(share * planes, planes)], held.at[q], load_sem.at[q])
        loads[q].start()

    field[...] = jnp.zeros_like(field)

    barrier = pltpu.get_barrier_semaphore()
    greet = [(b + (1 << k) * (1 - 2 * ((b // (1 << k)) % 2)), s) for k in range(stages)]
    across = [(b, (s + k) % spaces) for k in range(1, spaces)]
    greet += across
    for peer in greet:
        pl.semaphore_signal(barrier, inc=1, device_id=peer, device_id_type=MESH)

    for q in range(bands):
        loads[q].wait()

    weights = [occ_ref[k] for k in range(groups)]

    def density(c, low, high):
        def body(i, _):
            position = low + i // part
            plane = i % part
            offset = permuted(position, orders[c], stages)
            total = jnp.zeros((rows, lanes), jnp.float32)
            for k in range(groups):
                wave = held[offset, k, c * part + plane].astype(jnp.float32)
                total = total + (weights[k] * wave) * wave
            acc[c, position, plane] = total
            return 0
        lax.fori_loop(0, (high - low) * part, body, 0)

    def hop(c, stage):
        half = bands >> (stage + 1)
        bit = 1 << orders[c][stage]
        peer = b + bit * (1 - 2 * ((b // bit) % 2))
        return pltpu.make_async_remote_copy(
            src_ref=acc.at[c, pl.ds(half, half)], dst_ref=got.at[c, pl.ds(half, half)],
            send_sem=rs_send.at[c, stage], recv_sem=rs_recv.at[c, stage],
            device_id=(peer, s), device_id_type=MESH)

    hops = {(c, t): hop(c, t) for c in range(chunks) for t in range(stages)}
    for c in range(chunks):
        density(c, bands // 2, bands)
        if c == 0:
            pl.semaphore_wait(barrier, len(greet))
        hops[c, 0].start()
    for c in range(chunks):
        density(c, 0, bands // 2)

    scale = 4.0 * math.pi / bands_total
    order = sorted(hops, key=lambda ct: (ct[1], ct[0]))
    for c, t in order:
        half = bands >> (t + 1)
        hops[c, t].wait_recv()

        if t + 1 < stages:
            quarter = half // 2

            def add(i, _):
                position, plane = i // part, i % part
                acc[c, position, plane] = acc[c, position, plane] + got[c, half + position, plane]
                return 0
            lax.fori_loop(quarter * part, half * part, add, 0)
            hops[c, t + 1].start()
            lax.fori_loop(0, quarter * part, add, 0)
        else:
            if c == 0:
                for peer in across:
                    pl.semaphore_signal(ready, inc=1, device_id=peer, device_id_type=MESH)
            for plane in range(part):
                field[DEEP + c * part + plane, EDGE:EDGE + rows] = scale * (
                    acc[c, 0, plane] + got[c, 1, plane])

    def span(d, size, width, halo):
        if d > 0:
            return size + halo - width, halo - width
        return halo, size + halo

    pl.semaphore_wait(ready, len(across))
    halos = []
    for i, (db, ds) in enumerate(DIRECTIONS):
        deep = planes if not db else (DEEP if (db, ds) == (-1, 0) else CORNER)
        wide = EDGE if ds else rows
        src_p, dst_p = span(db, planes, deep, DEEP) if db else (DEEP, DEEP)
        src_r, dst_r = span(ds, rows, wide, EDGE) if ds else (EDGE, EDGE)
        to = ((b + db + bands) % bands, (s + ds + spaces) % spaces)
        copy = pltpu.make_async_remote_copy(
            src_ref=field.at[pl.ds(src_p, deep), pl.ds(src_r, wide)],
            dst_ref=field.at[pl.ds(dst_p, deep), pl.ds(dst_r, wide)],
            send_sem=halo_send.at[i], recv_sem=halo_recv.at[i],
            device_id=to, device_id_type=MESH)

        def inside(x, y, db=db, ds=ds):
            ok = None
            for d, v, n in ((db, x, bands), (ds, y, spaces)):
                if d:
                    here = (v + d >= 0) & (v + d < n)
                    ok = here if ok is None else ok & here
            return ok
        sends = inside(b, s)
        takes = None
        for d, v, n in ((db, b, bands), (ds, s, spaces)):
            if d:
                here = (v - d >= 0) & (v - d < n)
                takes = here if takes is None else takes & here
        pl.when(sends)(copy.start)
        halos.append((copy, sends, takes))
    for copy, sends, takes in halos:
        pl.when(takes)(copy.wait_recv)
    for copy, sends, takes in halos:
        pl.when(sends)(copy.wait_send)

    row = lax.broadcasted_iota(jnp.int32, (tall, lanes), 0)
    lane = lax.broadcasted_iota(jnp.int32, (tall, lanes), 1)
    low_row = jnp.where(s == 0, EDGE, 0)
    high_row = jnp.where(s == spaces - 1, EDGE + rows, tall)
    rows_in = ((row >= low_row) & (row < high_row)).astype(jnp.float32)
    near, far = -4.0 / 3.0, 1.0 / 12.0
    lane_terms = [(shift % lanes, jnp.where((lane - shift >= 0) & (lane - shift < lanes), w, 0.0))
                  for shift, w in ((1, near), (-1, near), (2, far), (-2, far))]
    low_plane = jnp.where(b == 0, DEEP, 0)
    high_plane = jnp.where(b == bands - 1, DEEP + planes, planes + 2 * DEEP)

    def apply(ref, p, forward=False):
        v = ref[p]
        if forward:
            ones, twos = 2.0 * ref[p + 1], 2.0 * ref[p + 2]
        else:
            ones, twos = ref[p - 1] + ref[p + 1], ref[p - 2] + ref[p + 2]
        ones = ones + pltpu.roll(v, 1, 0) + pltpu.roll(v, tall - 1, 0)
        twos = twos + pltpu.roll(v, 2, 0) + pltpu.roll(v, tall - 2, 0)
        total = 7.5 * v + near * ones + far * twos
        for shift, coefficient in lane_terms:
            total = total + coefficient * pltpu.roll(v, shift, 1)
        return total

    def step(src, dst):
        def body(p, _):
            here = jnp.where((p >= low_plane) & (p < high_plane), 1.0, 0.0)
            dst[p] = apply(src, p) * (rows_in * here)
            return 0
        return body

    lax.fori_loop(2 * REACH, planes + 2 * DEEP - REACH, step(field, first), 0)
    lax.fori_loop(DEEP, planes + 2 * DEEP - 2 * REACH, step(first, second), 0)

    def fold(x):
        x = x[EDGE:EDGE + rows]
        total = x[0:8]
        for k in range(8, rows, 8):
            total = total + x[k:k + 8]
        return total

    def moments(p, sums):
        w0, w1, w2 = field[p], first[p], second[p]
        w3 = apply(second, p, forward=True)
        terms = (w0 * w0, w0 * w1, w1 * w1, w1 * w2, w2 * w2, w2 * w3)
        return tuple(x + fold(y) for x, y in zip(sums, terms))

    sums = lax.fori_loop(DEEP, DEEP + planes, moments,
                         tuple(jnp.zeros((8, lanes), jnp.float32) for _ in range(6)))
    slot = lax.broadcasted_iota(jnp.int32, (1, lanes), 1)
    packed = jnp.zeros((1, lanes), jnp.float32)
    for k, x in enumerate(sums):
        value = jnp.sum(jnp.sum(x, axis=0, keepdims=True), axis=1, keepdims=True)
        packed = packed + jnp.where(slot == k, value, 0.0)
    mine[...] = packed
    me = b * spaces + s
    copies = []
    for k in range(bands * spaces - 1, 0, -1):
        to = ((b + k // spaces) % bands, (s + k % spaces) % spaces)
        copies.append(pltpu.make_async_remote_copy(
            src_ref=mine, dst_ref=theirs.at[me], send_sem=mb_send.at[k], recv_sem=mb_recv.at[k],
            device_id=to, device_id_type=MESH))
        copies[-1].start()
    theirs[me] = packed
    for copy in copies:
        copy.wait_recv()
    total = jnp.sum(theirs[...], axis=0)
    mu = [jnp.sum(jnp.where(slot == k, total, 0.0), axis=1, keepdims=True) for k in range(6)]

    def form(c, shift):
        value = None
        for i in range(len(c)):
            for j in range(i, len(c)):
                term = c[i] * c[j] * mu[i + j + shift]
                term = term if i == j else 2.0 * term
                value = term if value is None else value + term
        return value

    alpha0 = mu[0] / mu[1]
    r1 = [jnp.ones_like(alpha0), -alpha0]
    rr1 = form(r1, 0)
    beta0 = rr1 / mu[0]
    d1 = [1.0 + beta0, -alpha0]
    alpha1 = rr1 / form(d1, 1)
    r2 = [r1[0], r1[1] - alpha1 * d1[0], -alpha1 * d1[1]]
    rr2 = form(r2, 0)
    beta1 = rr2 / rr1
    d2 = [r2[0] + beta1 * d1[0], r2[1] + beta1 * d1[1], r2[2]]
    alpha2 = rr2 / form(d2, 1)
    c0 = alpha0 + alpha1 * d1[0] + alpha2 * d2[0]
    c1 = alpha1 * d1[1] + alpha2 * d2[1]
    c2 = alpha2 * d2[2]

    for p in range(planes):
        at = (DEEP + p, slice(EDGE, EDGE + rows))
        out_ref[p] = c0 * field[at] + c1 * first[at] + c2 * second[at]

    for c, t in order:
        hops[c, t].wait_send()
    for copy in copies:
        copy.wait_send()


def solution(mesh):
    bands, spaces = mesh.shape["band"], mesh.shape["space"]
    stages = bands.bit_length() - 1

    def local(orbitals, occupations):
        groups, length, rows, lanes = orbitals.shape
        planes = length // bands
        chunks = 4
        part = planes // chunks
        forward = list(range(stages))
        half = stages // 2
        swapped = forward[half:half + 1] + forward[:half] + forward[half + 1:]
        orders = [forward if c % 2 == 0 else swapped for c in range(chunks)]
        body = functools.partial(kernel, bands, spaces, groups, groups * bands, chunks, orders)
        tall, deep = rows + 2 * EDGE, planes + 2 * DEEP
        f32 = jnp.float32
        return pl.pallas_call(
            body,
            out_shape=jax.ShapeDtypeStruct((planes, rows, lanes), f32),
            in_specs=[pl.BlockSpec(memory_space=pltpu.SMEM), pl.BlockSpec(memory_space=pltpu.HBM)],
            out_specs=pl.BlockSpec(memory_space=pltpu.VMEM),
            scratch_shapes=[
                pltpu.VMEM((bands, groups, planes, rows, lanes), orbitals.dtype),
                pltpu.VMEM((chunks, bands, part, rows, lanes), f32),
                pltpu.VMEM((chunks, bands, part, rows, lanes), f32),
                pltpu.VMEM((deep, tall, lanes), f32),
                pltpu.VMEM((deep, tall, lanes), f32),
                pltpu.VMEM((deep, tall, lanes), f32),
                pltpu.VMEM((1, lanes), f32),
                pltpu.VMEM((bands * spaces, 1, lanes), f32),
                pltpu.SemaphoreType.DMA((bands,)),
                pltpu.SemaphoreType.DMA((chunks, stages)),
                pltpu.SemaphoreType.DMA((chunks, stages)),
                pltpu.SemaphoreType.DMA((len(DIRECTIONS),)),
                pltpu.SemaphoreType.DMA((len(DIRECTIONS),)),
                pltpu.SemaphoreType.DMA((bands * spaces,)),
                pltpu.SemaphoreType.DMA((bands * spaces,)),
                pltpu.SemaphoreType.REGULAR,
            ],
            compiler_params=pltpu.CompilerParams(
                collective_id=0, has_side_effects=True, vmem_limit_bytes=67043328),
        )(occupations, orbitals)

    in_specs = (P("band", None, "space", None), P("band"))
    out_specs = P("band", "space", None)
    return jax.shard_map(local, mesh=mesh, in_specs=in_specs, out_specs=out_specs, check_vma=False)
```
